32 devices in a mesh: group: 2 (over x), expert: 16 (over z, y, core).
Axes of the slice: x: 2, y: 2, z: 4, core: 2. Of those that a mesh axis runs over, the one named last changes fastest.
Arguments:
- query: bfloat16 [32, 2048], P(('group', 'expert')), parts along dimension 0, may hold values from -600 to 600
- key_new: bfloat16 [32, 2048], P(('group', 'expert')), parts along dimension 0, may hold values from -6 to 6
- value_new: bfloat16 [32, 2048], P(('group', 'expert')), parts along dimension 0, may hold values from -6 to 6
- key_cache: bfloat16 [32, 256, 2048], P(('group', 'expert')), parts along dimension 0, may hold values from -6 to 6
- value_cache: bfloat16 [32, 256, 2048], P(('group', 'expert')), parts along dimension 0, may hold values from -6 to 6
- lengths: int32 [32], P(('group', 'expert')), parts along dimension 0, may hold values from 1 to 256
- hidden: bfloat16 [32, 2048], P(('group', 'expert')), parts along dimension 0, may hold values from -6 to 6
- routes: int32 [32], P('group'), parts along dimension 0, may hold values from 0 to 31, as said below
- w_out: bfloat16 [2048, 2048], P(None, 'expert'), may hold values from -0.125 to 0.125
- ln_gain: bfloat16 [2048], replicated, may hold values from 0.099609375 to 1.8984375
- router: bfloat16 [2048, 32], replicated, may hold values from -0.125 to 0.125
- shared_up: bfloat16 [2048, 8192], P(None, 'expert'), may hold values from -0.125 to 0.125
- shared_down: bfloat16 [8192, 2048], P('expert'), may hold values from -0.0625 to 0.0625
- expert_up: bfloat16 [2048, 131072], P(None, 'expert'), may hold values from -0.125 to 0.125
- expert_down: bfloat16 [131072, 2048], P('expert'), may hold values from -0.09375 to 0.09375
Outputs:
- layer_out: bfloat16 [32, 2048], P(('group', 'expert')), parts along dimension 0
The draws below stay inside these ranges and needn't reach their ends.
There are 2 independent parts, one for each index of `group`. The reference program is written for one: setup_inputs(seed, part) draws one part's arguments, and reference() takes and returns one part's arrays. A program takes and returns all parts, laid end to end along the dimension named above; an argument that names none is the same for every part. Nothing has to cross between parts.
Inputs may be any that keep to these rules, and one draw needn't show every extreme that they name: `routes`: no expert is named by more than 2 tokens of the group, and in every draw some expert is named by exactly 2.
All inputs are finite; a program needn't handle non-finite values.
Results may differ from the reference program's by a relative error of at most 0.0085.
Values may be sent and summed in bfloat16 or wider, within the bound.
A program may use at most 128 MiB of HBM per device.

```python
import math
import jax
import jax.numpy as jnp
from jax import lax

D = 2048
HEADS = 16
HEAD_DIM = 128
FF = 4096
EXPERTS = 32
SHARED_FF = 8192
CACHE = 256
S = 16
CAP = 2


def draw_query(key, part):
    base = jnp.clip(jax.random.normal(key, (S, D), jnp.float32), -6.0, 6.0)
    return base.astype(jnp.bfloat16)


def draw_routes(key, part):
    order_key = jax.random.fold_in(key, 11)
    hot_key = jax.random.fold_in(key, 12)
    second_key = jax.random.fold_in(key, 13)
    count_key = jax.random.fold_in(key, 14)
    shuffle_key = jax.random.fold_in(key, 15)
    offset_key = jax.random.fold_in(key, 16)
    token_order = jax.random.permutation(order_key, S)
    hottest = jax.random.randint(hot_key, (), 0, EXPERTS)
    second = (hottest + 1 + jax.random.randint(second_key, (), 0, EXPERTS - 1)) % EXPERTS
    second_count = jax.random.randint(count_key, (), 1, CAP + 1)
    expert_index = jnp.arange(EXPERTS, dtype=jnp.int32)
    shuffled = jax.random.permutation(shuffle_key, EXPERTS).astype(jnp.int32)
    shuffled = jnp.where(expert_index == hottest, EXPERTS, shuffled)
    shuffled = jnp.where(expert_index == second, EXPERTS + 1, shuffled)
    others = jnp.argsort(shuffled, stable=True).astype(jnp.int32)
    offset = jax.random.randint(offset_key, (), 0, EXPERTS - 2)
    position = jnp.arange(S, dtype=jnp.int32)
    remaining = (position - CAP - second_count + offset) % (EXPERTS - 2)
    chosen = jnp.where(position < CAP, hottest, jnp.where(position < CAP + second_count, second, others[remaining]))
    return jnp.zeros((S,), jnp.int32).at[token_order].set(chosen.astype(jnp.int32))


def place_ends(entries, own_key, smallest, largest):
    shape = entries.shape
    place = [jax.random.randint(jax.random.fold_in(own_key, axis), (), 0, shape[axis]) for axis in range(len(shape))]
    entries = entries.at[tuple(place)].set(smallest)
    longest = shape.index(max(shape))
    place[longest] = (place[longest] + 1) % shape[longest]
    return entries.at[tuple(place)].set(largest)


def block_levels(own_key, shape, pieces, low, top_value):
    loudness = 1.0
    for dim, parts in pieces:
        heights = jax.random.uniform(jax.random.fold_in(jax.random.fold_in(own_key, 6), dim), (parts,), jnp.float32, low / len(pieces), top_value / len(pieces))
        loudness = loudness * jnp.repeat(jnp.exp(heights), shape[dim] // parts).reshape((-1,) + (1,) * (len(shape) - 1 - dim))
    return loudness


def gaussian(stream_key, shape, width, bound, pieces=(), held_as=jnp.bfloat16):
    drawn = jax.random.normal(stream_key, shape, jnp.float32) * width
    if len(pieces) > 0:
        drawn = block_levels(stream_key, shape, pieces, -0.22, 0.18) * drawn
    return jnp.clip(drawn, min=-bound, max=bound).astype(held_as)


def setup_inputs(seed: int = 0, part: int = 0) -> dict:
    keys = jax.random.split(jax.random.key(seed), 16)
    part_splits = jax.random.split(jax.random.fold_in(keys[15], part), 16)
    return {
        "query": draw_query(jax.random.fold_in(jax.random.fold_in(keys[15], part), 71), part),
        "key_new": gaussian(part_splits[1], (S, D), 1.0, 6.0, ((0, 16),)),
        "value_new": gaussian(part_splits[2], (S, D), 1.0, 6.0, ((0, 16),)),
        "key_cache": gaussian(part_splits[3], (S, CACHE, D), 1.0, 6.0, ((0, 16),)),
        "value_cache": gaussian(part_splits[4], (S, CACHE, D), 1.0, 6.0, ((0, 16),)),
        "lengths": place_ends(jax.random.randint(part_splits[5], (S,), 1, CACHE + 1), jax.random.fold_in(part_splits[5], 1), 1, CACHE).astype(jnp.int32),
        "hidden": gaussian(part_splits[6], (S, D), 1.0, 6.0, ((0, 16),)),
        "routes": draw_routes(jax.random.fold_in(jax.random.fold_in(keys[15], part), 71), part),
        "w_out": gaussian(keys[8], (D, D), D ** -0.5, 0.125, ((1, 16),)),
        "ln_gain": jnp.clip(1.0 + 0.18 * jax.random.normal(keys[9], (D,), jnp.float32), 0.099609375, 1.8984375).astype(jnp.bfloat16),
        "router": gaussian(keys[10], (D, EXPERTS), D ** -0.5, 0.125),
        "shared_up": gaussian(keys[11], (D, SHARED_FF), D ** -0.5, 0.125, ((1, 16),)),
        "shared_down": gaussian(keys[12], (SHARED_FF, D), SHARED_FF ** -0.5, 0.0625, ((0, 16),)),
        "expert_up": gaussian(keys[13], (D, EXPERTS * FF), D ** -0.5, 0.125, ((1, 16),)),
        "expert_down": gaussian(keys[14], (EXPERTS * FF, D), FF ** -0.5, 0.09375, ((0, 16),)),
    }


def attend_one(packed):
    query_row, key_rows, value_rows, key_self, value_self, valid = packed
    scale_factor = 1.0 / math.sqrt(HEAD_DIM)
    head_query = query_row.astype(jnp.float32).reshape(HEADS, HEAD_DIM)
    head_keys = key_rows.astype(jnp.float32).reshape(CACHE, HEADS, HEAD_DIM)
    head_values = value_rows.astype(jnp.float32).reshape(CACHE, HEADS, HEAD_DIM)
    scores = jnp.einsum('hd,chd->hc', head_query, head_keys) * scale_factor
    own_score = lax.optimization_barrier(jnp.sum(head_query * key_self.astype(jnp.float32).reshape(HEADS, HEAD_DIM), axis=1)) * scale_factor
    positions = jnp.arange(CACHE, dtype=jnp.int32)
    scores = jnp.where(positions[None, :] < valid, scores, -1e+30)
    top_score = jnp.maximum(lax.optimization_barrier(jnp.max(scores, axis=1)), own_score)
    weights = jnp.exp(scores - top_score[:, None])
    own_weight = jnp.exp(own_score - top_score)
    normalizer = lax.optimization_barrier(jnp.sum(weights, axis=1)) + own_weight
    weights = lax.optimization_barrier((weights / normalizer[:, None]).astype(jnp.bfloat16)).astype(jnp.float32)
    own_weight = lax.optimization_barrier((own_weight / normalizer).astype(jnp.bfloat16)).astype(jnp.float32)
    mixed_values = jnp.einsum('hc,chd->hd', weights, head_values)
    mixed_values = mixed_values + own_weight[:, None] * value_self.astype(jnp.float32).reshape(HEADS, HEAD_DIM)
    return mixed_values.reshape(D).astype(jnp.bfloat16)

def reference(query, key_new, value_new, key_cache, value_cache, lengths, hidden, routes, w_out, ln_gain, router, shared_up, shared_down, expert_up, expert_down):
    attended = lax.map(attend_one, (query, key_cache, value_cache, key_new, value_new, lengths))
    projected = jnp.dot(attended, w_out, preferred_element_type=jnp.float32).astype(jnp.bfloat16)
    projected = lax.optimization_barrier(projected).astype(jnp.float32)
    residual = hidden.astype(jnp.float32) + projected
    centered = residual - lax.optimization_barrier(jnp.mean(residual, axis=1, keepdims=True))
    variance = lax.optimization_barrier(jnp.mean(centered * centered, axis=1, keepdims=True))
    normed = (centered / jnp.sqrt(jnp.maximum(variance, 0.25)) * ln_gain.astype(jnp.float32)).astype(jnp.bfloat16)
    logits = jnp.dot(normed, router, preferred_element_type=jnp.float32)
    expert_ids = jnp.arange(EXPERTS, dtype=jnp.int32)
    chosen = lax.optimization_barrier(jnp.sum(jnp.where(routes[:, None] == expert_ids[None, :], logits, 0.0), axis=1))
    gate_value = jax.nn.sigmoid(chosen)
    shared_hidden = jax.nn.gelu(jnp.dot(normed, shared_up, preferred_element_type=jnp.float32), approximate=True).astype(jnp.bfloat16)
    shared_out = jnp.dot(shared_hidden, shared_down, preferred_element_type=jnp.float32)
    slot_ids = jnp.arange(CAP, dtype=jnp.int32)

    def one_expert(running, expert_id):
        member = routes == expert_id
        slot_rank = jnp.cumsum(member.astype(jnp.int32)) - 1
        placed = member[:, None] & (slot_rank[:, None] == slot_ids[None, :])
        picked = jnp.dot(placed.astype(jnp.bfloat16).T, normed, preferred_element_type=jnp.float32).astype(jnp.bfloat16)
        up_cols = lax.dynamic_slice_in_dim(expert_up, (expert_id * FF).astype(jnp.int32), FF, 1)
        down_rows = lax.dynamic_slice_in_dim(expert_down, (expert_id * FF).astype(jnp.int32), FF, 0)
        inner_act = jax.nn.gelu(jnp.dot(picked, up_cols, preferred_element_type=jnp.float32), approximate=True).astype(jnp.bfloat16)
        result = jnp.dot(inner_act, down_rows, preferred_element_type=jnp.float32)
        spread = placed.astype(jnp.float32) * gate_value[:, None]
        return (running + jnp.dot(spread, result, precision=lax.Precision.HIGHEST), None)
    expert_out, ignored = lax.scan(one_expert, jnp.zeros((S, D), jnp.float32), expert_ids)
    return (residual + shared_out + expert_out).astype(jnp.bfloat16)
```

```python
import functools
import math

import jax
import jax.numpy as jnp
from jax import lax
from jax.experimental import pallas as pl
from jax.experimental.pallas import tpu as pltpu
from jax.sharding import PartitionSpec as P

HEADS = 16
HEAD_DIM = 128
FF = 4096
EXPERTS = 32
CHUNK = 512
BLOCK = 512
EARLY = 3
PRIORITY = 1
TOGETHER = 4
GROUP_COLS = 1024
MESH = pl.DeviceIdType.MESH
F32 = jnp.float32
BF16 = jnp.bfloat16


def gelu(v):
    return 0.5 * v * (1.0 + jnp.tanh(math.sqrt(2.0 / math.pi) * (v + 0.044715 * (v * v * v))))


def kernel(
    replicas,
    n,
    lengths_hbm,
    routes_hbm,
    query_hbm,
    key_new_hbm,
    value_new_hbm,
    hidden_hbm,
    gain_hbm,
    keys_hbm,
    values_hbm,
    w_out_hbm,
    router_hbm,
    shared_up_hbm,
    shared_down_hbm,
    up_hbm,
    down_hbm,
    out_ref,
    lengths_ref,
    routes_all,
    query,
    key_new,
    value_new,
    hidden,
    gain,
    keys,
    values,
    w_out,
    router,
    shared_up,
    shared_down,
    up,
    down,
    attended_all,
    hidden_all,
    unfold,
    projected_all,
    inner,
    normed_ref,
    gate_ref,
    shared_ref,
    own_ref,
    terms_buf,
    send_buf,
    recv_buf,
    local_sem,
    up_sem,
    down_sem,
    send_sem,
    recv_sem,
):
    mine_g = lax.axis_index("group")
    me = lax.axis_index("expert")
    world = replicas * n
    rank = mine_g * n + me
    width = query.shape[1]
    units = up_hbm.shape[1]
    share = units // replicas
    chunk_cols = up.shape[2]
    up_chunks = up.shape[0]
    block_cols = down.shape[2]
    blocks = down.shape[0]
    piece = min(share, width)
    pieces = share // piece
    shared_units = shared_up_hbm.shape[1]
    shared_share = shared_up.shape[1]

    barrier = pltpu.get_barrier_semaphore()

    if shared_share == shared_units:
        shared_up_src, shared_down_src = shared_up_hbm, shared_down_hbm
    else:
        my_shared = pl.ds(pl.multiple_of(mine_g * shared_share, shared_share), shared_share)
        shared_up_src = shared_up_hbm.at[:, my_shared]
        shared_down_src = shared_down_hbm.at[my_shared, :]

    local = [
        pltpu.make_async_copy(src, dst, local_sem.at[i])
        for i, (src, dst) in enumerate(
            [
                (query_hbm, query),
                (key_new_hbm, key_new),
                (keys_hbm, keys),
                (values_hbm, values),
                (value_new_hbm, value_new),
                (hidden_hbm, hidden),
                (w_out_hbm, w_out),
                (gain_hbm, gain),
                (router_hbm, router),
                (shared_up_src, shared_up),
                (shared_down_src, shared_down),
                (lengths_hbm, lengths_ref),
                (routes_hbm, routes_all.at[mine_g]),
            ]
        )
    ]
    (
        query_copy,
        key_new_copy,
        keys_copy,
        values_copy,
        value_new_copy,
        hidden_copy,
        w_out_copy,
        gain_copy,
        router_copy,
        shared_up_copy,
        shared_down_copy,
        lengths_copy,
        routes_copy,
    ) = local

    def up_copy(chunk):
        first = mine_g * share + chunk * chunk_cols
        return pltpu.make_async_copy(
            up_hbm.at[:, pl.ds(pl.multiple_of(first, chunk_cols), chunk_cols)],
            up.at[chunk],
            up_sem.at[chunk],
        )

    def down_copy(block, part):
        first = mine_g * share + part * piece
        return pltpu.make_async_copy(
            down_hbm.at[
                pl.ds(pl.multiple_of(first, piece), piece),
                pl.ds(block * block_cols, block_cols),
            ],
            down.at[block, pl.ds(part * piece, piece), :],
            down_sem.at[block * pieces + part],
        )

    chunk_copies = [up_copy(c) for c in range(up_chunks)] + [
        down_copy(b, p) for b in range(blocks) for p in range(pieces)
    ]
    issued = 0

    def start_chunks(last):
        nonlocal issued
        while issued < min(last, len(chunk_copies)):
            chunk_copies[issued].start(priority=PRIORITY)
            issued += 1

    for copy in (query_copy, key_new_copy, keys_copy, values_copy, value_new_copy, hidden_copy, lengths_copy, routes_copy, w_out_copy):
        copy.start()
    start_chunks(EARLY)

    def place(peer):
        return {"group": peer // n, "expert": lax.rem(peer, n)}

    def greet(off, carry):
        pl.semaphore_signal(
            barrier, inc=1, device_id=place(lax.rem(rank + off, world)), device_id_type=MESH
        )
        return carry

    lax.fori_loop(1, world, greet, 0)

    rows = lax.broadcasted_iota(jnp.int32, (HEADS, width), 0)
    lanes = lax.broadcasted_iota(jnp.int32, (HEADS, width), 1)
    own_lane = lanes // HEAD_DIM == rows

    def fold(x):
        row = lax.broadcasted_iota(jnp.int32, (HEADS, HEAD_DIM), 0)
        taken = jnp.zeros((HEADS, HEAD_DIM), F32)
        for h in range(HEADS):
            taken = taken + jnp.where(row == h, x[:, h * HEAD_DIM : (h + 1) * HEAD_DIM], 0.0)
        return taken

    scale = 1.0 / math.sqrt(HEAD_DIM)
    query_copy.wait()
    key_new_copy.wait()
    spread_query = jnp.where(
        own_lane, jnp.broadcast_to(query[...].astype(F32), (HEADS, width)), 0.0
    )
    own_score = (
        jnp.sum(spread_query * key_new[...].astype(F32), axis=1, keepdims=True) * scale
    )
    spread_query = spread_query.astype(BF16)
    mine = pl.ds(pl.multiple_of(me * HEADS, HEADS), HEADS)
    hidden_copy.wait()
    hidden_all[mine_g, mine, :] = fold(
        jnp.broadcast_to(hidden[...].astype(F32), (HEADS, width))
    ).astype(BF16)
    keys_copy.wait()
    scores = (
        lax.dot_general(
            spread_query, keys[...], (((1,), (1,)), ((), ())), preferred_element_type=F32
        )
        * scale
    )
    lengths_copy.wait()
    values_copy.wait()
    value_new_copy.wait()
    for copy in (gain_copy, router_copy, shared_up_copy, shared_down_copy):
        copy.start()
    start_chunks(len(chunk_copies))

    position = lax.broadcasted_iota(jnp.int32, scores.shape, 1)
    scores = jnp.where(position < lengths_ref[0], scores, -1e30)
    top = jnp.maximum(jnp.max(scores, axis=1, keepdims=True), own_score)
    weights = jnp.exp(scores - top)
    own_weight = jnp.exp(own_score - top)
    normalizer = jnp.sum(weights, axis=1, keepdims=True) + own_weight
    weights = (weights / normalizer).astype(BF16)
    own_weight = (own_weight / normalizer).astype(BF16).astype(F32)
    mixed = jnp.dot(weights, values[...], preferred_element_type=F32)
    mixed = mixed + own_weight * value_new[...].astype(F32)
    attended_all[mine, :] = fold(mixed).astype(BF16)
    routes_copy.wait()

    pl.semaphore_wait(barrier, world - 1)

    def send(src, dst, sem, to):
        pltpu.make_async_remote_copy(
            src_ref=src,
            dst_ref=dst,
            send_sem=send_sem.at[sem],
            recv_sem=recv_sem.at[sem],
            device_id=to,
            device_id_type=MESH,
        ).start()

    def send_group(ref, sem):
        def step(off, carry):
            send(ref, ref, sem, {"expert": lax.rem(me + off, n)})
            return carry

        lax.fori_loop(1, n, step, 0)

    def send_twins(ref, sem):
        for off in range(1, replicas):
            send(ref, ref, sem, {"group": lax.rem(mine_g + off, replicas)})

    def send_others(ref, sem):
        for other in range(1, replicas):

            def step(off, carry, other=other):
                group = lax.rem(mine_g + other, replicas)
                send(ref, ref, sem, {"group": group, "expert": lax.rem(me + off, n)})
                return carry

            lax.fori_loop(0, n, step, 0)

    def await_bytes(ref, sem):
        pltpu.make_async_copy(ref, ref, sem).wait()

    attended_piece = attended_all.at[mine, :]
    send_group(attended_piece, 0)
    send_group(hidden_all.at[mine_g, mine, :], 1)
    send_twins(routes_all.at[mine_g], 2)

    others = pl.ds(0, (n - 1) * HEADS)
    token = lax.broadcasted_iota(jnp.int32, (world, 1), 0)
    await_bytes(hidden_all.at[0, others, :], recv_sem.at[1])
    send_twins(hidden_all.at[mine_g], 3)
    await_bytes(attended_all.at[others, :], recv_sem.at[0])
    unfold[pl.ds(0, n * HEADS), :] = attended_all[...].astype(F32)
    attended = jnp.concatenate(
        [unfold[pl.ds(h, n, stride=HEADS), :].astype(BF16) for h in range(HEADS)], axis=1
    )
    w_out_copy.wait()
    projected = jnp.dot(attended, w_out[...], preferred_element_type=F32).astype(BF16)
    cols = projected.shape[1]
    my_cols = pl.ds(pl.multiple_of(me * cols, cols), cols)
    if cols % 128 == 0:
        projected_all[mine_g, :, my_cols] = projected
        piece_ref = projected_all.at[mine_g, :, my_cols]
        near = projected_all.at[0, :, pl.ds(0, (n - 1) * cols)]
    else:
        projected_all[mine_g, me] = projected
        piece_ref = projected_all.at[mine_g, me]
        near = projected_all.at[0, pl.ds(0, n - 1)]
    far = projected_all.at[pl.ds(0, replicas - 1)]
    send_group(piece_ref, 4)
    send_others(piece_ref, 5)

    twins = pl.ds(0, replicas - 1)
    await_bytes(routes_all.at[twins], recv_sem.at[2])
    square = (n, n)
    on_diagonal = lax.broadcasted_iota(jnp.int32, square, 0) == lax.broadcasted_iota(
        jnp.int32, square, 1
    )
    chosen_expert = jnp.concatenate(
        [
            jnp.sum(
                jnp.where(on_diagonal, jnp.broadcast_to(routes_all[i].astype(F32), square), 0.0),
                axis=1,
                keepdims=True,
            )
            for i in range(replicas)
        ],
        axis=0,
    )
    gain_copy.wait()
    router_copy.wait()
    expert_ids = lax.broadcasted_iota(jnp.int32, (world, EXPERTS), 1).astype(F32)
    chosen_router = jnp.dot(
        jnp.where(chosen_expert == expert_ids, 1.0, 0.0).astype(BF16),
        router[...],
        preferred_element_type=F32,
    )
    await_bytes(hidden_all.at[twins], recv_sem.at[3])
    unfold[...] = hidden_all[...].reshape(world * HEADS, HEAD_DIM).astype(F32)
    every_hidden = jnp.concatenate(
        [unfold[pl.ds(h, world, stride=HEADS), :] for h in range(HEADS)], axis=1
    )
    await_bytes(near, recv_sem.at[4])
    await_bytes(far, recv_sem.at[5])
    if cols % 128 == 0:
        every_projected = projected_all[...].reshape(world, width).astype(F32)
    else:
        every_projected = jnp.concatenate(
            [
                jnp.concatenate([projected_all[i, d].astype(F32) for d in range(n)], axis=1)
                for i in range(replicas)
            ],
            axis=0,
        )
    residual = every_hidden + every_projected
    centered = residual - jnp.mean(residual, axis=1, keepdims=True)
    variance = jnp.mean(centered * centered, axis=1, keepdims=True)
    normed = (
        centered / jnp.sqrt(jnp.maximum(variance, 0.25)) * gain[...].astype(F32).reshape(1, width)
    ).astype(BF16)
    normed_ref[...] = normed
    own_ref[...] = jnp.sum(jnp.where(token == rank, residual, 0.0), axis=0, keepdims=True)
    chosen = jnp.sum(normed.astype(F32) * chosen_router, axis=1, keepdims=True)
    gate_ref[...] = 1.0 / (1.0 + jnp.exp(-chosen))

    shared_up_copy.wait()
    shared_act = gelu(jnp.dot(normed_ref[...], shared_up[...], preferred_element_type=F32))
    if shared_share == shared_units:
        unit = lax.broadcasted_iota(jnp.int32, shared_act.shape, 1)
        shared_act = jnp.where(unit // (shared_units // replicas) == mine_g, shared_act, 0.0)
    shared_ref[...] = shared_act.astype(BF16)

    together = math.gcd(TOGETHER, up_chunks)

    def up_step(step, carry):
        chunks = [step * together + i for i in range(together)]
        for chunk in chunks:
            up_copy(chunk).wait()
        for chunk in chunks:
            act = gelu(jnp.dot(normed_ref[...], up[chunk], preferred_element_type=F32))
            expert = (me * units + mine_g * share + chunk * chunk_cols) // FF
            inner[:, pl.ds(pl.multiple_of(chunk * chunk_cols, chunk_cols), chunk_cols)] = jnp.where(
                chosen_expert == expert.astype(F32), act, 0.0
            ).astype(BF16)
        return carry

    lax.fori_loop(0, up_chunks // together, up_step, 0)
    shared_down_copy.wait()

    group_rows = GROUP_COLS // 128
    groups = width // GROUP_COLS
    blocks_per_group = blocks // groups

    for group in range(groups):
        for index in range(blocks_per_group):
            block = group * blocks_per_group + index
            for part in range(pieces):
                down_copy(block, part).wait()
            acc = jnp.dot(inner[...], down[block], preferred_element_type=F32)
            shared = jnp.dot(
                shared_ref[...],
                shared_down[:, pl.ds(block * block_cols, block_cols)],
                preferred_element_type=F32,
            )
            terms = shared + gate_ref[...] * acc
            for k in range(block_cols // 128):
                row = index * (block_cols // 128) + k
                terms_buf[pl.ds(row, world, stride=group_rows), :] = terms[:, k * 128 : (k + 1) * 128]
        send_buf[group] = terms_buf[...].reshape(world, group_rows, 128).astype(BF16)

        def send_terms(off, carry, group=group):
            peer = lax.rem(rank + off, world)
            send(send_buf.at[group, peer], recv_buf.at[group, rank], 6 + group, place(peer))
            return carry

        lax.fori_loop(1, world, send_terms, 0)
        recv_buf[group, rank] = send_buf[group, rank]

    for group in range(groups):
        landed = recv_buf.at[group, pl.ds(0, world - 1)]
        await_bytes(landed, recv_sem.at[6 + group])
        summed = jnp.zeros((group_rows, 128), F32)
        for d in range(world):
            summed = summed + recv_buf[group, d].astype(F32)
        for j in range(group_rows):
            where = pl.ds(group * GROUP_COLS + j * 128, 128)
            out_ref[:, where] = (own_ref[:, where] + summed[j : j + 1, :]).astype(out_ref.dtype)

    await_bytes(attended_all.at[others, :], send_sem.at[0])
    await_bytes(hidden_all.at[0, others, :], send_sem.at[1])
    await_bytes(routes_all.at[twins], send_sem.at[2])
    await_bytes(hidden_all.at[twins], send_sem.at[3])
    await_bytes(near, send_sem.at[4])
    await_bytes(far, send_sem.at[5])
    for group in range(groups):
        sent = send_buf.at[group, pl.ds(0, world - 1)]
        await_bytes(sent, send_sem.at[6 + group])


def solution(mesh):
    n = mesh.shape["expert"]
    replicas = mesh.shape["group"]
    world = n * replicas

    def body(
        query,
        key_new,
        value_new,
        key_cache,
        value_cache,
        lengths,
        hidden,
        routes,
        w_out,
        ln_gain,
        router,
        shared_up,
        shared_down,
        expert_up,
        expert_down,
    ):
        assert query.shape[0] == 1
        width = query.shape[1]
        share = expert_up.shape[1] // replicas
        cache = key_cache.shape[1]
        shared_share = shared_up.shape[1] // replicas
        if shared_share % 128:
            shared_share = shared_up.shape[1]
        cols = w_out.shape[1]
        chunk_cols = min(CHUNK, share)
        up_chunks = share // chunk_cols
        blocks = width // BLOCK
        pieces = share // min(share, width)
        groups = width // GROUP_COLS
        rows_sent = GROUP_COLS // 128
        gathered = (replicas, n, width) if cols % 128 == 0 else (replicas, n, n, cols)
        vmem = pltpu.VMEM
        hbm = pl.BlockSpec(memory_space=pl.ANY)
        return pl.pallas_call(
            functools.partial(kernel, replicas, n),
            out_shape=pltpu.VMEM((1, width), BF16),
            in_specs=[hbm] * 15,
            out_specs=pl.BlockSpec(memory_space=pltpu.VMEM),
            scratch_shapes=[
                pltpu.SMEM(lengths.shape, jnp.int32),
                vmem((replicas, 1, n), jnp.int32),
                vmem((1, width), BF16),
                vmem((1, width), BF16),
                vmem((1, width), BF16),
                vmem((1, width), BF16),
                vmem((width,), BF16),
                vmem((cache, width), BF16),
                vmem((cache, width), BF16),
                vmem((width, cols), BF16),
                vmem((EXPERTS, width), BF16),
                vmem((width, shared_share), BF16),
                vmem((shared_share, width), BF16),
                vmem((up_chunks, width, chunk_cols), BF16),
                vmem((blocks, share, BLOCK), BF16),
                vmem((n * HEADS, HEAD_DIM), BF16),
                vmem((replicas, n * HEADS, HEAD_DIM), BF16),
                vmem((world * HEADS, HEAD_DIM), F32),
                vmem(gathered, BF16),
                vmem((world, share), BF16),
                vmem((world, width), BF16),
                vmem((world, 1), F32),
                vmem((world, shared_share), BF16),
                vmem((1, width), F32),
                vmem((world * rows_sent, 128), F32),
                vmem((groups, world, rows_sent, 128), BF16),
                vmem((groups, world, rows_sent, 128), BF16),
                pltpu.SemaphoreType.DMA((13,)),
                pltpu.SemaphoreType.DMA((up_chunks,)),
                pltpu.SemaphoreType.DMA((blocks * pieces,)),
                pltpu.SemaphoreType.DMA((6 + groups,)),
                pltpu.SemaphoreType.DMA((6 + groups,)),
            ],
            compiler_params=pltpu.CompilerParams(
                collective_id=0, has_side_effects=True, vmem_limit_bytes=66_900_000
            ),
        )(
            lengths,
            routes.reshape(1, n),
            query,
            key_new,
            value_new,
            hidden,
            ln_gain,
            key_cache.reshape(cache, width),
            value_cache.reshape(cache, width),
            w_out,
            router.T,
            shared_up,
            shared_down,
            expert_up,
            expert_down,
        )

    rows = P(("group", "expert"), None)
    placed = (
        rows,
        rows,
        rows,
        P(("group", "expert"), None, None),
        P(("group", "expert"), None, None),
        P(("group", "expert")),
        rows,
        P("group"),
        P(None, "expert"),
        P(),
        P(),
        P(None, "expert"),
        P("expert", None),
        P(None, "expert"),
        P("expert", None),
    )
    return jax.shard_map(body, mesh=mesh, in_specs=placed, out_specs=rows, check_vma=False)
```

```python
import functools
import math

import jax
import jax.numpy as jnp
from jax import lax
from jax.experimental import pallas as pl
from jax.experimental.pallas import tpu as pltpu
from jax.sharding import PartitionSpec as P

HEADS = 16
HEAD_DIM = 128
FF = 4096
EXPERTS = 32
CHUNK = 512
BLOCK = 512
EARLY = 3
PRIORITY = 1
UNROLL = 32
MOST_ROUTED = 8
GROUP_COLS = 1024
MESH = pl.DeviceIdType.MESH
F32 = jnp.float32
BF16 = jnp.bfloat16


def gelu(v):
    return 0.5 * v * (1.0 + jnp.tanh(math.sqrt(2.0 / math.pi) * (v + 0.044715 * (v * v * v))))


def kernel(
    replicas,
    n,
    lengths_hbm,
    routes_hbm,
    query_hbm,
    key_new_hbm,
    value_new_hbm,
    hidden_hbm,
    gain_hbm,
    keys_hbm,
    values_hbm,
    w_out_hbm,
    router_hbm,
    shared_up_hbm,
    shared_down_hbm,
    up_hbm,
    down_hbm,
    out_ref,
    lengths_ref,
    routes_all,
    query,
    key_new,
    value_new,
    hidden,
    gain,
    keys,
    values,
    w_out,
    router,
    shared_up,
    shared_down,
    up,
    down,
    attended_all,
    hidden_all,
    unfold,
    projected_all,
    picked_hidden,
    guest_hidden,
    picked_projected,
    guest_projected,
    guests_ref,
    inner,
    normed_ref,
    gate_ref,
    shared_ref,
    own_ref,
    terms_buf,
    send_buf,
    recv_buf,
    local_sem,
    up_sem,
    down_sem,
    send_sem,
    recv_sem,
):
    mine_g = lax.axis_index("group")
    me = lax.axis_index("expert")
    world = replicas * n
    rank = mine_g * n + me
    width = query.shape[1]
    units = up_hbm.shape[1]
    share = units // replicas
    chunk_cols = up.shape[2]
    up_chunks = up.shape[0]
    block_cols = down.shape[2]
    blocks = down.shape[0]
    piece = min(share, width)
    pieces = share // piece
    slots = guest_hidden.shape[1]
    served = guests_ref.shape[0]
    cols = w_out.shape[1]

    def expert_of(group, device):
        return (device * units + group * share) // FF

    barrier = pltpu.get_barrier_semaphore()

    local = [
        pltpu.make_async_copy(src, dst, local_sem.at[i])
        for i, (src, dst) in enumerate(
            [
                (query_hbm, query),
                (key_new_hbm, key_new),
                (keys_hbm, keys),
                (values_hbm, values),
                (value_new_hbm, value_new),
                (hidden_hbm, hidden),
                (w_out_hbm, w_out),
                (gain_hbm, gain),
                (router_hbm, router),
                (shared_up_hbm, shared_up),
                (shared_down_hbm, shared_down),
                (lengths_hbm, lengths_ref),
                (routes_hbm, routes_all.at[mine_g]),
            ]
        )
    ]
    (
        query_copy,
        key_new_copy,
        keys_copy,
        values_copy,
        value_new_copy,
        hidden_copy,
        w_out_copy,
        gain_copy,
        router_copy,
        shared_up_copy,
        shared_down_copy,
        lengths_copy,
        routes_copy,
    ) = local

    def up_copy(chunk):
        first = mine_g * share + chunk * chunk_cols
        return pltpu.make_async_copy(
            up_hbm.at[:, pl.ds(pl.multiple_of(first, chunk_cols), chunk_cols)],
            up.at[chunk],
            up_sem.at[chunk],
        )

    def down_copy(block, part):
        first = mine_g * share + part * piece
        return pltpu.make_async_copy(
            down_hbm.at[
                pl.ds(pl.multiple_of(first, piece), piece),
                pl.ds(block * block_cols, block_cols),
            ],
            down.at[block, pl.ds(part * piece, piece), :],
            down_sem.at[block * pieces + part],
        )

    chunk_copies = [up_copy(c) for c in range(up_chunks)] + [shared_down_copy] + [
        down_copy(b, p) for b in range(blocks) for p in range(pieces)
    ]
    issued = 0

    def start_chunks(last):
        nonlocal issued
        while issued < min(last, len(chunk_copies)):
            chunk_copies[issued].start(priority=PRIORITY)
            issued += 1

    for copy in (query_copy, key_new_copy, keys_copy, values_copy, value_new_copy, hidden_copy, lengths_copy, routes_copy, w_out_copy):
        copy.start()
    start_chunks(EARLY)

    def place(peer):
        return {"group": peer // n, "expert": lax.rem(peer, n)}

    def greet(off, carry):
        pl.semaphore_signal(
            barrier, inc=1, device_id=place(lax.rem(rank + off, world)), device_id_type=MESH
        )
        return carry

    lax.fori_loop(1, world, greet, 0)

    rows = lax.broadcasted_iota(jnp.int32, (HEADS, width), 0)
    lanes = lax.broadcasted_iota(jnp.int32, (HEADS, width), 1)
    own_lane = lanes // HEAD_DIM == rows

    def fold(x):
        row = lax.broadcasted_iota(jnp.int32, (HEADS, HEAD_DIM), 0)
        taken = jnp.zeros((HEADS, HEAD_DIM), F32)
        for h in range(HEADS):
            taken = taken + jnp.where(row == h, x[:, h * HEAD_DIM : (h + 1) * HEAD_DIM], 0.0)
        return taken

    scale = 1.0 / math.sqrt(HEAD_DIM)
    query_copy.wait()
    key_new_copy.wait()
    spread_query = jnp.where(
        own_lane, jnp.broadcast_to(query[...].astype(F32), (HEADS, width)), 0.0
    )
    own_score = (
        jnp.sum(spread_query * key_new[...].astype(F32), axis=1, keepdims=True) * scale
    )
    spread_query = spread_query.astype(BF16)
    mine = pl.ds(pl.multiple_of(me * HEADS, HEADS), HEADS)
    hidden_copy.wait()
    hidden_all[mine, :] = fold(
        jnp.broadcast_to(hidden[...].astype(F32), (HEADS, width))
    ).astype(BF16)
    keys_copy.wait()
    scores = (
        lax.dot_general(
            spread_query, keys[...], (((1,), (1,)), ((), ())), preferred_element_type=F32
        )
        * scale
    )
    lengths_copy.wait()
    values_copy.wait()
    value_new_copy.wait()
    for copy in (gain_copy, router_copy, shared_up_copy):
        copy.start()
    start_chunks(len(chunk_copies))

    position = lax.broadcasted_iota(jnp.int32, scores.shape, 1)
    scores = jnp.where(position < lengths_ref[0], scores, -1e30)
    top = jnp.maximum(jnp.max(scores, axis=1, keepdims=True), own_score)
    weights = jnp.exp(scores - top)
    own_weight = jnp.exp(own_score - top)
    normalizer = jnp.sum(weights, axis=1, keepdims=True) + own_weight
    weights = (weights / normalizer).astype(BF16)
    own_weight = (own_weight / normalizer).astype(BF16).astype(F32)
    mixed = jnp.dot(weights, values[...], preferred_element_type=F32)
    mixed = mixed + own_weight * value_new[...].astype(F32)
    attended_all[mine, :] = fold(mixed).astype(BF16)
    routes_copy.wait()

    pl.semaphore_wait(barrier, world - 1)

    def send(src, dst, sem, to):
        pltpu.make_async_remote_copy(
            src_ref=src,
            dst_ref=dst,
            send_sem=send_sem.at[sem],
            recv_sem=recv_sem.at[sem],
            device_id=to,
            device_id_type=MESH,
        ).start()

    def loop(count, step):
        if count <= UNROLL:
            for i in range(count):
                step(i)
        else:

            def body(i, carry):
                step(i)
                return carry

            lax.fori_loop(0, count, body, 0)

    def other_group(off):
        return lax.rem(mine_g + off, replicas)

    def other_device(i):
        return i + jnp.where(i >= me, 1, 0)

    def send_group(ref, sem):
        loop(n - 1, lambda i: send(ref, ref, sem, {"expert": other_device(i)}))

    def await_bytes(ref, sem):
        pltpu.make_async_copy(ref, ref, sem).wait()

    attended_piece = attended_all.at[mine, :]
    send_group(attended_piece, 0)
    send_group(hidden_all.at[mine, :], 1)
    for off in range(1, replicas):
        send(routes_all.at[mine_g], routes_all.at[mine_g], 2, {"group": other_group(off)})

    square = (n, n)
    down_index = lax.broadcasted_iota(jnp.int32, square, 0)
    across_index = lax.broadcasted_iota(jnp.int32, square, 1)

    def placed(group):
        across = jnp.broadcast_to(routes_all[group].astype(F32), square)
        route = jnp.sum(
            jnp.where(down_index == across_index, across, 0.0), axis=1, keepdims=True
        )
        same = jnp.broadcast_to(route, square) == across
        slot_down = jnp.sum(
            jnp.where(same & (across_index < down_index), 1.0, 0.0), axis=1, keepdims=True
        )
        slot_across = jnp.sum(
            jnp.where(same & (down_index < across_index), 1.0, 0.0), axis=0, keepdims=True
        )
        return route, slot_down, across[0:1, :], slot_across

    route, slot_down, route_across, slot_across = placed(mine_g)

    def picks(expert, slot):
        wanted = jnp.broadcast_to(route_across, expert.shape) == expert.astype(F32)
        ranked = jnp.broadcast_to(slot_across, slot.shape) == slot.astype(F32)
        return jnp.where(wanted & ranked, 1.0, 0.0).astype(BF16)

    def picks_for_device(group):
        slot = lax.broadcasted_iota(jnp.int32, (served, n), 0)
        expert = jnp.full((served, n), expert_of(group, me), jnp.int32)
        return picks(expert, jnp.where(slot < slots, slot, n))

    def picks_for_group(group):
        row = lax.broadcasted_iota(jnp.int32, (n * slots, n), 0)
        return picks(expert_of(group, row // slots), row - row // slots * slots)

    own_picks = picks_for_device(mine_g)
    twin_picks = [picks_for_device(other_group(off)) for off in range(1, replicas)]
    group_picks = [picks_for_group(other_group(off)) for off in range(1, replicas)]
    guests_ref[...] = jnp.zeros(guests_ref.shape, F32)

    def unfolded(folded):
        unfold[...] = folded[...].astype(F32)
        return [unfold[pl.ds(h, n, stride=HEADS), :].astype(BF16) for h in range(HEADS)]

    others = pl.ds(0, (n - 1) * HEADS)
    twins = pl.ds(0, replicas - 1)
    w_out_copy.wait()
    await_bytes(attended_all.at[others, :], recv_sem.at[0])
    attended = jnp.concatenate(unfolded(attended_all), axis=1)
    projected = jnp.dot(attended, w_out[...], preferred_element_type=F32).astype(BF16)
    my_cols = pl.ds(pl.multiple_of(me * cols, cols), cols)
    if cols % 128 == 0:
        projected_all[:, my_cols] = projected
        piece_ref = projected_all.at[:, my_cols]
        near = projected_all.at[:, pl.ds(0, (n - 1) * cols)]
    else:
        projected_all[me] = projected
        piece_ref = projected_all.at[me]
        near = projected_all.at[pl.ds(0, n - 1)]
    for off in range(1, replicas):
        picked = jnp.dot(group_picks[off - 1], projected, preferred_element_type=F32)
        for j in range(n):
            picked_projected[off - 1, j] = picked[j * slots : (j + 1) * slots, :]
        group = other_group(off)
        loop(
            n,
            lambda j: send(
                picked_projected.at[off - 1, j],
                guest_projected.at[off - 1, me],
                4,
                {"group": group, "expert": j},
            ),
        )
    send_group(piece_ref, 3)
    await_bytes(hidden_all.at[others, :], recv_sem.at[1])
    every_hidden = jnp.concatenate(unfolded(hidden_all), axis=1)
    for off in range(1, replicas):
        picked_hidden[off - 1] = jnp.dot(
            twin_picks[off - 1], every_hidden, preferred_element_type=F32
        )[:slots, :]
        send(
            picked_hidden.at[off - 1],
            guest_hidden.at[off - 1],
            5,
            {"group": other_group(off)},
        )

    await_bytes(routes_all.at[twins], recv_sem.at[2])
    my_expert = expert_of(mine_g, me).astype(F32)

    def places(their_route, their_slot):
        here = their_route == my_expert
        return [jnp.where(here & (their_slot == float(k)), 1.0, 0.0) for k in range(slots)]

    token_places = [places(route, slot_down)]
    for off in range(1, replicas):
        their_route, their_slot, _, _ = placed(other_group(replicas - off))
        token_places.append(places(their_route, their_slot))
    gain_copy.wait()
    router_copy.wait()
    gain_row = gain[...].astype(F32).reshape(1, width)
    router_row = jnp.sum(
        jnp.where(
            lax.broadcasted_iota(jnp.int32, (EXPERTS, width), 0) == expert_of(mine_g, me),
            router[...].astype(F32),
            0.0,
        ),
        axis=0,
        keepdims=True,
    )

    def norm(residual):
        centered = residual - jnp.mean(residual, axis=1, keepdims=True)
        variance = jnp.mean(centered * centered, axis=1, keepdims=True)
        return centered / jnp.sqrt(jnp.maximum(variance, 0.25)) * gain_row

    token = lax.broadcasted_iota(jnp.int32, (n, 1), 0)
    shared_up_copy.wait()
    for chunk in range(up_chunks):
        up_copy(chunk).wait()
    await_bytes(near, recv_sem.at[3])
    if cols % 128 == 0:
        every_projected = projected_all[...].astype(F32)
    else:
        every_projected = jnp.concatenate([projected_all[d].astype(F32) for d in range(n)], axis=1)
    residual = every_hidden.astype(F32) + every_projected
    normed = norm(residual).astype(BF16)
    own_served = jnp.dot(own_picks, normed, preferred_element_type=F32)
    own_ref[...] = jnp.sum(jnp.where(token == me, residual, 0.0), axis=0, keepdims=True)
    shared_ref[...] = gelu(
        jnp.dot(normed, shared_up[...], preferred_element_type=F32)
    ).astype(BF16)

    await_bytes(guest_hidden, recv_sem.at[5])
    await_bytes(guest_projected, recv_sem.at[4])
    for off in range(1, replicas):
        theirs = jnp.concatenate([guest_projected[off - 1, d] for d in range(n)], axis=1)
        guests_ref[pl.ds(off * slots, slots), :] = norm(guest_hidden[off - 1] + theirs)
    everyone = (own_served + guests_ref[...]).astype(BF16)
    normed_ref[...] = everyone
    chosen = jnp.sum(everyone.astype(F32) * router_row, axis=1, keepdims=True)
    gate_ref[...] = 1.0 / (1.0 + jnp.exp(-chosen))
    for chunk in range(up_chunks):
        act = gelu(jnp.dot(normed_ref[...], up[chunk], preferred_element_type=F32))
        inner[:, pl.ds(chunk * chunk_cols, chunk_cols)] = act.astype(BF16)

    group_rows = GROUP_COLS // 128
    groups = width // GROUP_COLS
    blocks_per_group = blocks // groups
    shared_down_copy.wait()

    for group in range(groups):
        half = blocks_per_group * pieces
        for copy in chunk_copies[up_chunks + 1 + group * half : up_chunks + 1 + (group + 1) * half]:
            copy.wait()
        for index in range(blocks_per_group):
            block = group * blocks_per_group + index
            acc = gate_ref[...] * jnp.dot(inner[...], down[block], preferred_element_type=F32)
            terms = []
            for side in range(replicas):
                if side == 0:
                    total = jnp.dot(
                        shared_ref[...],
                        shared_down[:, pl.ds(block * block_cols, block_cols)],
                        preferred_element_type=F32,
                    )
                else:
                    total = jnp.zeros((n, block_cols), F32)
                for k in range(slots):
                    row = side * slots + k
                    total = total + token_places[side][k] * acc[row : row + 1, :]
                terms.append(total)
            for side in range(replicas):
                for k in range(block_cols // 128):
                    row = side * n * group_rows + index * (block_cols // 128) + k
                    terms_buf[pl.ds(row, n, stride=group_rows), :] = terms[side][
                        :, k * 128 : (k + 1) * 128
                    ]
        send_buf[group] = terms_buf[...].reshape(world, group_rows, 128).astype(BF16)

        def send_terms(i, group=group):
            def to(side, device):
                where = side * n
                send(
                    send_buf.at[group, where + device],
                    recv_buf.at[group, where + me],
                    6 + group,
                    {"group": other_group(replicas - side), "expert": device},
                )

            for side in range(1, replicas):
                to(side, i)
            if isinstance(i, int):
                if i < n - 1:
                    to(0, other_device(i))
            else:

                @pl.when(i < n - 1)
                def _():
                    to(0, other_device(i))

        loop(n, send_terms)
        recv_buf[group, me] = send_buf[group, me]

    for group in range(groups):
        landed = recv_buf.at[group, pl.ds(0, world - 1)]
        await_bytes(landed, recv_sem.at[6 + group])
        summed = jnp.zeros((group_rows, 128), F32)
        for d in range(world):
            summed = summed + recv_buf[group, d].astype(F32)
        for j in range(group_rows):
            where = pl.ds(group * GROUP_COLS + j * 128, 128)
            out_ref[:, where] = (own_ref[:, where] + summed[j : j + 1, :]).astype(out_ref.dtype)

    await_bytes(attended_all.at[others, :], send_sem.at[0])
    await_bytes(hidden_all.at[others, :], send_sem.at[1])
    await_bytes(routes_all.at[twins], send_sem.at[2])
    await_bytes(near, send_sem.at[3])
    await_bytes(guest_projected, send_sem.at[4])
    await_bytes(guest_hidden, send_sem.at[5])
    for group in range(groups):
        sent = send_buf.at[group, pl.ds(0, world - 1)]
        await_bytes(sent, send_sem.at[6 + group])


def solution(mesh):
    n = mesh.shape["expert"]
    replicas = mesh.shape["group"]
    world = n * replicas

    def body(
        query,
        key_new,
        value_new,
        key_cache,
        value_cache,
        lengths,
        hidden,
        routes,
        w_out,
        ln_gain,
        router,
        shared_up,
        shared_down,
        expert_up,
        expert_down,
    ):
        assert query.shape[0] == 1
        width = query.shape[1]
        share = expert_up.shape[1] // replicas
        cache = key_cache.shape[1]
        shared_units = shared_up.shape[1]
        cols = w_out.shape[1]
        slots = max(1, n // MOST_ROUTED)
        served = -(-slots * replicas // 16) * 16
        chunk_cols = min(CHUNK, share)
        up_chunks = share // chunk_cols
        blocks = width // BLOCK
        pieces = share // min(share, width)
        groups = width // GROUP_COLS
        rows_sent = GROUP_COLS // 128
        gathered = (n, width) if cols % 128 == 0 else (n, n, cols)
        vmem = pltpu.VMEM
        hbm = pl.BlockSpec(memory_space=pl.ANY)
        return pl.pallas_call(
            functools.partial(kernel, replicas, n),
            out_shape=pltpu.VMEM((1, width), BF16),
            in_specs=[hbm] * 15,
            out_specs=pl.BlockSpec(memory_space=pltpu.VMEM),
            scratch_shapes=[
                pltpu.SMEM(lengths.shape, jnp.int32),
                vmem((replicas, 1, n), jnp.int32),
                vmem((1, width), BF16),
                vmem((1, width), BF16),
                vmem((1, width), BF16),
                vmem((1, width), BF16),
                vmem((width,), BF16),
                vmem((cache, width), BF16),
                vmem((cache, width), BF16),
                vmem((width, cols), BF16),
                vmem((EXPERTS, width), BF16),
                vmem((width, shared_units), BF16),
                vmem((shared_units, width), BF16),
                vmem((up_chunks, width, chunk_cols), BF16),
                vmem((blocks, share, BLOCK), BF16),
                vmem((n * HEADS, HEAD_DIM), BF16),
                vmem((n * HEADS, HEAD_DIM), BF16),
                vmem((n * HEADS, HEAD_DIM), F32),
                vmem(gathered, BF16),
                vmem((replicas - 1, slots, width), F32),
                vmem((replicas - 1, slots, width), F32),
                vmem((replicas - 1, n, slots, cols), F32),
                vmem((replicas - 1, n, slots, cols), F32),
                vmem((served, width), F32),
                vmem((served, share), BF16),
                vmem((served, width), BF16),
                vmem((served, 1), F32),
                vmem((n, shared_units), BF16),
                vmem((1, width), F32),
                vmem((world * rows_sent, 128), F32),
                vmem((groups, world, rows_sent, 128), BF16),
                vmem((groups, world, rows_sent, 128), BF16),
                pltpu.SemaphoreType.DMA((13,)),
                pltpu.SemaphoreType.DMA((up_chunks,)),
                pltpu.SemaphoreType.DMA((blocks * pieces,)),
                pltpu.SemaphoreType.DMA((6 + groups,)),
                pltpu.SemaphoreType.DMA((6 + groups,)),
            ],
            compiler_params=pltpu.CompilerParams(
                collective_id=0, has_side_effects=True, vmem_limit_bytes=66_900_000
            ),
        )(
            lengths,
            routes.reshape(1, n),
            query,
            key_new,
            value_new,
            hidden,
            ln_gain,
            key_cache.reshape(cache, width),
            value_cache.reshape(cache, width),
            w_out,
            router.T,
            shared_up,
            shared_down,
            expert_up,
            expert_down,
        )

    rows = P(("group", "expert"), None)
    placed = (
        rows,
        rows,
        rows,
        P(("group", "expert"), None, None),
        P(("group", "expert"), None, None),
        P(("group", "expert")),
        rows,
        P("group"),
        P(None, "expert"),
        P(),
        P(),
        P(None, "expert"),
        P("expert", None),
        P(None, "expert"),
        P("expert", None),
    )
    return jax.shard_map(body, mesh=mesh, in_specs=placed, out_specs=rows, check_vma=False)
```

```python
import functools
import math

import jax
import jax.numpy as jnp
from jax import lax
from jax.experimental import pallas as pl
from jax.experimental.pallas import tpu as pltpu
from jax.sharding import PartitionSpec as P

HEADS = 16
HEAD_DIM = 128
FF = 4096
EXPERTS = 32
CHUNK = 512
BLOCK = 512
EARLY = 99
PRIORITY = 1
UNROLL = 32
MOST_ROUTED = 8
GROUP_COLS = 2048
MESH = pl.DeviceIdType.MESH
F32 = jnp.float32
BF16 = jnp.bfloat16


def gelu(v):
    return 0.5 * v * (1.0 + jnp.tanh(math.sqrt(2.0 / math.pi) * (v + 0.044715 * (v * v * v))))


def kernel(
    replicas,
    n,
    lengths_hbm,
    routes_hbm,
    query_hbm,
    key_new_hbm,
    value_new_hbm,
    hidden_hbm,
    gain_hbm,
    keys_hbm,
    values_hbm,
    w_out_hbm,
    router_hbm,
    shared_up_hbm,
    shared_down_hbm,
    up_hbm,
    down_hbm,
    out_ref,
    lengths_ref,
    routes_all,
    query,
    key_new,
    value_new,
    hidden,
    gain,
    keys,
    values,
    w_out,
    router,
    shared_up,
    shared_down,
    up,
    down,
    attended_all,
    hidden_all,
    unfold,
    projected_all,
    picked_hidden,
    guest_hidden,
    picked_projected,
    guest_projected,
    guests_ref,
    inner,
    normed_ref,
    gate_ref,
    shared_ref,
    own_ref,
    terms_buf,
    send_buf,
    recv_buf,
    local_sem,
    up_sem,
    down_sem,
    send_sem,
    recv_sem,
):
    mine_g = lax.axis_index("group")
    me = lax.axis_index("expert")
    world = replicas * n
    rank = mine_g * n + me
    width = query.shape[1]
    units = up_hbm.shape[1]
    share = units // replicas
    chunk_cols = up.shape[2]
    up_chunks = up.shape[0]
    block_cols = down.shape[2]
    blocks = down.shape[0]
    piece = min(share, width)
    pieces = share // piece
    slots = guest_hidden.shape[1]
    served = guests_ref.shape[0]
    cols = w_out.shape[1]

    def expert_of(group, device):
        return (device * units + group * share) // FF

    barrier = pltpu.get_barrier_semaphore()

    local = [
        pltpu.make_async_copy(src, dst, local_sem.at[i])
        for i, (src, dst) in enumerate(
            [
                (query_hbm, query),
                (key_new_hbm, key_new),
                (keys_hbm, keys),
                (values_hbm, values),
                (value_new_hbm, value_new),
                (hidden_hbm, hidden),
                (w_out_hbm, w_out),
                (gain_hbm, gain),
                (router_hbm, router),
                (shared_up_hbm, shared_up),
                (shared_down_hbm, shared_down),
                (lengths_hbm, lengths_ref),
                (routes_hbm, routes_all.at[mine_g]),
            ]
        )
    ]
    (
        query_copy,
        key_new_copy,
        keys_copy,
        values_copy,
        value_new_copy,
        hidden_copy,
        w_out_copy,
        gain_copy,
        router_copy,
        shared_up_copy,
        shared_down_copy,
        lengths_copy,
        routes_copy,
    ) = local

    def up_copy(chunk):
        first = mine_g * share + chunk * chunk_cols
        return pltpu.make_async_copy(
            up_hbm.at[:, pl.ds(pl.multiple_of(first, chunk_cols), chunk_cols)],
            up.at[chunk],
            up_sem.at[chunk],
        )

    def down_copy(block, part):
        first = mine_g * share + part * piece
        return pltpu.make_async_copy(
            down_hbm.at[
                pl.ds(pl.multiple_of(first, piece), piece),
                pl.ds(block * block_cols, block_cols),
            ],
            down.at[block, pl.ds(part * piece, piece), :],
            down_sem.at[block * pieces + part],
        )

    chunk_copies = [up_copy(c) for c in range(up_chunks)] + [shared_down_copy] + [
        down_copy(b, p) for b in range(blocks) for p in range(pieces)
    ]
    issued = 0

    def start_chunks(last):
        nonlocal issued
        while issued < min(last, len(chunk_copies)):
            chunk_copies[issued].start(priority=PRIORITY)
            issued += 1

    for copy in (query_copy, key_new_copy, keys_copy, values_copy, value_new_copy, hidden_copy, lengths_copy, routes_copy, w_out_copy, gain_copy, router_copy, shared_up_copy):
        copy.start()
    start_chunks(EARLY)

    def place(peer):
        return {"group": peer // n, "expert": lax.rem(peer, n)}

    def greet(off, carry):
        pl.semaphore_signal(
            barrier, inc=1, device_id=place(lax.rem(rank + off, world)), device_id_type=MESH
        )
        return carry

    lax.fori_loop(1, world, greet, 0)

    rows = lax.broadcasted_iota(jnp.int32, (HEADS, width), 0)
    lanes = lax.broadcasted_iota(jnp.int32, (HEADS, width), 1)
    own_lane = lanes // HEAD_DIM == rows

    def fold(x):
        row = lax.broadcasted_iota(jnp.int32, (HEADS, HEAD_DIM), 0)
        taken = jnp.zeros((HEADS, HEAD_DIM), F32)
        for h in range(HEADS):
            taken = taken + jnp.where(row == h, x[:, h * HEAD_DIM : (h + 1) * HEAD_DIM], 0.0)
        return taken

    scale = 1.0 / math.sqrt(HEAD_DIM)
    query_copy.wait()
    key_new_copy.wait()
    spread_query = jnp.where(
        own_lane, jnp.broadcast_to(query[...].astype(F32), (HEADS, width)), 0.0
    )
    own_score = (
        jnp.sum(spread_query * key_new[...].astype(F32), axis=1, keepdims=True) * scale
    )
    spread_query = spread_query.astype(BF16)
    mine = pl.ds(pl.multiple_of(me * HEADS, HEADS), HEADS)
    hidden_copy.wait()
    hidden_all[mine, :] = fold(
        jnp.broadcast_to(hidden[...].astype(F32), (HEADS, width))
    ).astype(BF16)
    keys_copy.wait()
    scores = (
        lax.dot_general(
            spread_query, keys[...], (((1,), (1,)), ((), ())), preferred_element_type=F32
        )
        * scale
    )
    lengths_copy.wait()
    values_copy.wait()
    value_new_copy.wait()
    start_chunks(len(chunk_copies))

    position = lax.broadcasted_iota(jnp.int32, scores.shape, 1)
    scores = jnp.where(position < lengths_ref[0], scores, -1e30)
    top = jnp.maximum(jnp.max(scores, axis=1, keepdims=True), own_score)
    weights = jnp.exp(scores - top)
    own_weight = jnp.exp(own_score - top)
    normalizer = jnp.sum(weights, axis=1, keepdims=True) + own_weight
    weights = (weights / normalizer).astype(BF16)
    own_weight = (own_weight / normalizer).astype(BF16).astype(F32)
    mixed = jnp.dot(weights, values[...], preferred_element_type=F32)
    mixed = mixed + own_weight * value_new[...].astype(F32)
    attended_all[mine, :] = fold(mixed).astype(BF16)
    routes_copy.wait()

    pl.semaphore_wait(barrier, world - 1)

    def send(src, dst, sem, to):
        pltpu.make_async_remote_copy(
            src_ref=src,
            dst_ref=dst,
            send_sem=send_sem.at[sem],
            recv_sem=recv_sem.at[sem],
            device_id=to,
            device_id_type=MESH,
        ).start()

    def loop(count, step):
        if count <= UNROLL:
            for i in range(count):
                step(i)
        else:

            def body(i, carry):
                step(i)
                return carry

            lax.fori_loop(0, count, body, 0)

    def other_group(off):
        return lax.rem(mine_g + off, replicas)

    def other_device(i):
        return i + jnp.where(i >= me, 1, 0)

    def send_group(ref, sem):
        loop(n - 1, lambda i: send(ref, ref, sem, {"expert": other_device(i)}))

    def await_bytes(ref, sem):
        pltpu.make_async_copy(ref, ref, sem).wait()

    attended_piece = attended_all.at[mine, :]
    send_group(attended_piece, 0)
    send_group(hidden_all.at[mine, :], 1)
    for off in range(1, replicas):
        send(routes_all.at[mine_g], routes_all.at[mine_g], 2, {"group": other_group(off)})

    square = (n, n)
    down_index = lax.broadcasted_iota(jnp.int32, square, 0)
    across_index = lax.broadcasted_iota(jnp.int32, square, 1)

    def placed(group):
        across = jnp.broadcast_to(routes_all[group].astype(F32), square)
        route = jnp.sum(
            jnp.where(down_index == across_index, across, 0.0), axis=1, keepdims=True
        )
        same = jnp.broadcast_to(route, square) == across
        slot_down = jnp.sum(
            jnp.where(same & (across_index < down_index), 1.0, 0.0), axis=1, keepdims=True
        )
        slot_across = jnp.sum(
            jnp.where(same & (down_index < across_index), 1.0, 0.0), axis=0, keepdims=True
        )
        return route, slot_down, across[0:1, :], slot_across

    route, slot_down, route_across, slot_across = placed(mine_g)

    def picks(expert, slot):
        wanted = jnp.broadcast_to(route_across, expert.shape) == expert.astype(F32)
        ranked = jnp.broadcast_to(slot_across, slot.shape) == slot.astype(F32)
        return jnp.where(wanted & ranked, 1.0, 0.0).astype(BF16)

    def picks_for_device(group):
        slot = lax.broadcasted_iota(jnp.int32, (served, n), 0)
        expert = jnp.full((served, n), expert_of(group, me), jnp.int32)
        return picks(expert, jnp.where(slot < slots, slot, n))

    def picks_for_group(group):
        row = lax.broadcasted_iota(jnp.int32, (n * slots, n), 0)
        return picks(expert_of(group, row // slots), row - row // slots * slots)

    own_picks = picks_for_device(mine_g)
    twin_picks = [picks_for_device(other_group(off)) for off in range(1, replicas)]
    group_picks = [picks_for_group(other_group(off)) for off in range(1, replicas)]
    guests_ref[...] = jnp.zeros(guests_ref.shape, F32)

    def unfolded(folded):
        unfold[...] = folded[...].astype(F32)
        return [unfold[pl.ds(h, n, stride=HEADS), :].astype(BF16) for h in range(HEADS)]

    others = pl.ds(0, (n - 1) * HEADS)
    twins = pl.ds(0, replicas - 1)
    w_out_copy.wait()
    await_bytes(attended_all.at[others, :], recv_sem.at[0])
    attended = jnp.concatenate(unfolded(attended_all), axis=1)
    projected = jnp.dot(attended, w_out[...], preferred_element_type=F32).astype(BF16)
    my_cols = pl.ds(pl.multiple_of(me * cols, cols), cols)
    if cols % 128 == 0:
        projected_all[:, my_cols] = projected
        piece_ref = projected_all.at[:, my_cols]
        near = projected_all.at[:, pl.ds(0, (n - 1) * cols)]
    else:
        projected_all[me] = projected
        piece_ref = projected_all.at[me]
        near = projected_all.at[pl.ds(0, n - 1)]
    for off in range(1, replicas):
        picked = jnp.dot(group_picks[off - 1], projected, preferred_element_type=F32)
        for j in range(n):
            picked_projected[off - 1, j] = picked[j * slots : (j + 1) * slots, :]
        group = other_group(off)
        loop(
            n,
            lambda j: send(
                picked_projected.at[off - 1, j],
                guest_projected.at[off - 1, me],
                4,
                {"group": group, "expert": j},
            ),
        )
    send_group(piece_ref, 3)
    await_bytes(hidden_all.at[others, :], recv_sem.at[1])
    every_hidden = jnp.concatenate(unfolded(hidden_all), axis=1)
    for off in range(1, replicas):
        picked_hidden[off - 1] = jnp.dot(
            twin_picks[off - 1], every_hidden, preferred_element_type=F32
        )[:slots, :]
        send(
            picked_hidden.at[off - 1],
            guest_hidden.at[off - 1],
            5,
            {"group": other_group(off)},
        )

    await_bytes(routes_all.at[twins], recv_sem.at[2])
    my_expert = expert_of(mine_g, me).astype(F32)

    def places(their_route, their_slot):
        here = their_route == my_expert
        return [jnp.where(here & (their_slot == float(k)), 1.0, 0.0) for k in range(slots)]

    token_places = [places(route, slot_down)]
    for off in range(1, replicas):
        their_route, their_slot, _, _ = placed(other_group(replicas - off))
        token_places.append(places(their_route, their_slot))
    gain_copy.wait()
    router_copy.wait()
    gain_row = gain[...].astype(F32).reshape(1, width)
    router_row = jnp.sum(
        jnp.where(
            lax.broadcasted_iota(jnp.int32, (EXPERTS, width), 0) == expert_of(mine_g, me),
            router[...].astype(F32),
            0.0,
        ),
        axis=0,
        keepdims=True,
    )

    def norm(residual):
        centered = residual - jnp.mean(residual, axis=1, keepdims=True)
        variance = jnp.mean(centered * centered, axis=1, keepdims=True)
        return centered / jnp.sqrt(jnp.maximum(variance, 0.25)) * gain_row

    token = lax.broadcasted_iota(jnp.int32, (n, 1), 0)
    shared_up_copy.wait()
    for chunk in range(up_chunks):
        up_copy(chunk).wait()
    await_bytes(near, recv_sem.at[3])
    if cols % 128 == 0:
        every_projected = projected_all[...].astype(F32)
    else:
        every_projected = jnp.concatenate([projected_all[d].astype(F32) for d in range(n)], axis=1)
    residual = every_hidden.astype(F32) + every_projected
    normed = norm(residual).astype(BF16)
    own_served = jnp.dot(own_picks, normed, preferred_element_type=F32)
    own_ref[...] = jnp.sum(jnp.where(token == me, residual, 0.0), axis=0, keepdims=True)
    shared_ref[...] = gelu(
        jnp.dot(normed, shared_up[...], preferred_element_type=F32)
    ).astype(BF16)

    await_bytes(guest_hidden, recv_sem.at[5])
    await_bytes(guest_projected, recv_sem.at[4])
    for off in range(1, replicas):
        theirs = jnp.concatenate([guest_projected[off - 1, d] for d in range(n)], axis=1)
        guests_ref[pl.ds(off * slots, slots), :] = norm(guest_hidden[off - 1] + theirs)
    everyone = (own_served + guests_ref[...]).astype(BF16)
    normed_ref[...] = everyone
    chosen = jnp.sum(everyone.astype(F32) * router_row, axis=1, keepdims=True)
    gate_ref[...] = 1.0 / (1.0 + jnp.exp(-chosen))
    for chunk in range(up_chunks):
        act = gelu(jnp.dot(normed_ref[...], up[chunk], preferred_element_type=F32))
        inner[:, pl.ds(chunk * chunk_cols, chunk_cols)] = act.astype(BF16)

    group_rows = GROUP_COLS // 128
    groups = width // GROUP_COLS
    blocks_per_group = blocks // groups
    shared_down_copy.wait()

    for group in range(groups):
        half = blocks_per_group * pieces
        for copy in chunk_copies[up_chunks + 1 + group * half : up_chunks + 1 + (group + 1) * half]:
            copy.wait()
        for index in range(blocks_per_group):
            block = group * blocks_per_group + index
            acc = gate_ref[...] * jnp.dot(inner[...], down[block], preferred_element_type=F32)
            terms = []
            for side in range(replicas):
                if side == 0:
                    total = jnp.dot(
                        shared_ref[...],
                        shared_down[:, pl.ds(block * block_cols, block_cols)],
                        preferred_element_type=F32,
                    )
                else:
                    total = jnp.zeros((n, block_cols), F32)
                for k in range(slots):
                    row = side * slots + k
                    total = total + token_places[side][k] * acc[row : row + 1, :]
                terms.append(total)
            for side in range(replicas):
                for k in range(block_cols // 128):
                    row = side * n * group_rows + index * (block_cols // 128) + k
                    terms_buf[pl.ds(row, n, stride=group_rows), :] = terms[side][
                        :, k * 128 : (k + 1) * 128
                    ]
        send_buf[group] = terms_buf[...].reshape(world, group_rows, 128).astype(BF16)

        def send_terms(i, group=group):
            def to(side, device):
                where = side * n
                send(
                    send_buf.at[group, where + device],
                    recv_buf.at[group, where + me],
                    6 + group,
                    {"group": other_group(replicas - side), "expert": device},
                )

            for side in range(1, replicas):
                to(side, i)
            if isinstance(i, int):
                if i < n - 1:
                    to(0, other_device(i))
            else:

                @pl.when(i < n - 1)
                def _():
                    to(0, other_device(i))

        loop(n, send_terms)
        recv_buf[group, me] = send_buf[group, me]

    for group in range(groups):
        landed = recv_buf.at[group, pl.ds(0, world - 1)]
        await_bytes(landed, recv_sem.at[6 + group])
        summed = jnp.zeros((group_rows, 128), F32)
        for d in range(world):
            summed = summed + recv_buf[group, d].astype(F32)
        for j in range(group_rows):
            where = pl.ds(group * GROUP_COLS + j * 128, 128)
            out_ref[:, where] = (own_ref[:, where] + summed[j : j + 1, :]).astype(out_ref.dtype)

    await_bytes(attended_all.at[others, :], send_sem.at[0])
    await_bytes(hidden_all.at[others, :], send_sem.at[1])
    await_bytes(routes_all.at[twins], send_sem.at[2])
    await_bytes(near, send_sem.at[3])
    await_bytes(guest_projected, send_sem.at[4])
    await_bytes(guest_hidden, send_sem.at[5])
    for group in range(groups):
        sent = send_buf.at[group, pl.ds(0, world - 1)]
        await_bytes(sent, send_sem.at[6 + group])


def solution(mesh):
    n = mesh.shape["expert"]
    replicas = mesh.shape["group"]
    world = n * replicas

    def body(
        query,
        key_new,
        value_new,
        key_cache,
        value_cache,
        lengths,
        hidden,
        routes,
        w_out,
        ln_gain,
        router,
        shared_up,
        shared_down,
        expert_up,
        expert_down,
    ):
        assert query.shape[0] == 1
        width = query.shape[1]
        share = expert_up.shape[1] // replicas
        cache = key_cache.shape[1]
        shared_units = shared_up.shape[1]
        cols = w_out.shape[1]
        slots = max(1, n // MOST_ROUTED)
        served = -(-slots * replicas // 16) * 16
        chunk_cols = min(CHUNK, share)
        up_chunks = share // chunk_cols
        blocks = width // BLOCK
        pieces = share // min(share, width)
        groups = width // GROUP_COLS
        rows_sent = GROUP_COLS // 128
        gathered = (n, width) if cols % 128 == 0 else (n, n, cols)
        vmem = pltpu.VMEM
        hbm = pl.BlockSpec(memory_space=pl.ANY)
        return pl.pallas_call(
            functools.partial(kernel, replicas, n),
            out_shape=pltpu.VMEM((1, width), BF16),
            in_specs=[hbm] * 15,
            out_specs=pl.BlockSpec(memory_space=pltpu.VMEM),
            scratch_shapes=[
                pltpu.SMEM(lengths.shape, jnp.int32),
                vmem((replicas, 1, n), jnp.int32),
                vmem((1, width), BF16),
                vmem((1, width), BF16),
                vmem((1, width), BF16),
                vmem((1, width), BF16),
                vmem((width,), BF16),
                vmem((cache, width), BF16),
                vmem((cache, width), BF16),
                vmem((width, cols), BF16),
                vmem((EXPERTS, width), BF16),
                vmem((width, shared_units), BF16),
                vmem((shared_units, width), BF16),
                vmem((up_chunks, width, chunk_cols), BF16),
                vmem((blocks, share, BLOCK), BF16),
                vmem((n * HEADS, HEAD_DIM), BF16),
                vmem((n * HEADS, HEAD_DIM), BF16),
                vmem((n * HEADS, HEAD_DIM), F32),
                vmem(gathered, BF16),
                vmem((replicas - 1, slots, width), F32),
                vmem((replicas - 1, slots, width), F32),
                vmem((replicas - 1, n, slots, cols), F32),
                vmem((replicas - 1, n, slots, cols), F32),
                vmem((served, width), F32),
                vmem((served, share), BF16),
                vmem((served, width), BF16),
                vmem((served, 1), F32),
                vmem((n, shared_units), BF16),
                vmem((1, width), F32),
                vmem((world * rows_sent, 128), F32),
                vmem((groups, world, rows_sent, 128), BF16),
                vmem((groups, world, rows_sent, 128), BF16),
                pltpu.SemaphoreType.DMA((13,)),
                pltpu.SemaphoreType.DMA((up_chunks,)),
                pltpu.SemaphoreType.DMA((blocks * pieces,)),
                pltpu.SemaphoreType.DMA((6 + groups,)),
                pltpu.SemaphoreType.DMA((6 + groups,)),
            ],
            compiler_params=pltpu.CompilerParams(
                collective_id=0, has_side_effects=True, vmem_limit_bytes=66_900_000
            ),
        )(
            lengths,
            routes.reshape(1, n),
            query,
            key_new,
            value_new,
            hidden,
            ln_gain,
            key_cache.reshape(cache, width),
            value_cache.reshape(cache, width),
            w_out,
            router.T,
            shared_up,
            shared_down,
            expert_up,
            expert_down,
        )

    rows = P(("group", "expert"), None)
    placed = (
        rows,
        rows,
        rows,
        P(("group", "expert"), None, None),
        P(("group", "expert"), None, None),
        P(("group", "expert")),
        rows,
        P("group"),
        P(None, "expert"),
        P(),
        P(),
        P(None, "expert"),
        P("expert", None),
        P(None, "expert"),
        P("expert", None),
    )
    return jax.shard_map(body, mesh=mesh, in_specs=placed, out_specs=rows, check_vma=False)
```

```python
import functools
import math

import jax
import jax.numpy as jnp
from jax import lax
from jax.experimental import pallas as pl
from jax.experimental.pallas import tpu as pltpu
from jax.sharding import PartitionSpec as P

HEADS = 16
HEAD_DIM = 128
FF = 4096
EXPERTS = 32
CHUNK = 512
BLOCK = 512
EARLY = 99
PRIORITY = 1
UNROLL = 32
MOST_ROUTED = 8
GROUP_COLS = 2048
MESH = pl.DeviceIdType.MESH
F32 = jnp.float32
BF16 = jnp.bfloat16


def gelu(v):
    return 0.5 * v * (1.0 + jnp.tanh(math.sqrt(2.0 / math.pi) * (v + 0.044715 * (v * v * v))))


def kernel(
    replicas,
    n,
    lengths_hbm,
    routes_hbm,
    query_hbm,
    key_new_hbm,
    value_new_hbm,
    hidden_hbm,
    gain_hbm,
    keys_hbm,
    values_hbm,
    w_out_hbm,
    router_hbm,
    shared_up_hbm,
    shared_down_hbm,
    up_hbm,
    down_hbm,
    out_ref,
    lengths_ref,
    routes_all,
    query,
    key_new,
    value_new,
    hidden,
    gain,
    keys,
    values,
    w_out,
    router,
    shared_up,
    shared_down,
    up,
    down,
    attended_all,
    hidden_all,
    unfold,
    projected_all,
    picked_hidden,
    guest_hidden,
    picked_projected,
    guest_projected,
    guests_ref,
    inner,
    normed_ref,
    gate_ref,
    shared_ref,
    own_ref,
    terms_buf,
    send_buf,
    recv_buf,
    local_sem,
    up_sem,
    down_sem,
    send_sem,
    recv_sem,
    ready_sem,
):
    mine_g = lax.axis_index("group")
    me = lax.axis_index("expert")
    world = replicas * n
    rank = mine_g * n + me
    width = query.shape[1]
    units = up_hbm.shape[1]
    share = units // replicas
    chunk_cols = up.shape[2]
    up_chunks = up.shape[0]
    block_cols = down.shape[2]
    blocks = down.shape[0]
    piece = min(share, width)
    pieces = share // piece
    slots = guest_hidden.shape[1]
    served = guests_ref.shape[0]
    cols = w_out.shape[1]

    def expert_of(group, device):
        return (device * units + group * share) // FF

    barrier = pltpu.get_barrier_semaphore()

    local = [
        pltpu.make_async_copy(src, dst, local_sem.at[i])
        for i, (src, dst) in enumerate(
            [
                (query_hbm, query),
                (key_new_hbm, key_new),
                (keys_hbm, keys),
                (values_hbm, values),
                (value_new_hbm, value_new),
                (hidden_hbm, hidden),
                (w_out_hbm, w_out),
                (gain_hbm, gain),
                (router_hbm, router),
                (shared_up_hbm, shared_up),
                (shared_down_hbm, shared_down),
                (lengths_hbm, lengths_ref),
                (routes_hbm, routes_all.at[mine_g]),
            ]
        )
    ]
    (
        query_copy,
        key_new_copy,
        keys_copy,
        values_copy,
        value_new_copy,
        hidden_copy,
        w_out_copy,
        gain_copy,
        router_copy,
        shared_up_copy,
        shared_down_copy,
        lengths_copy,
        routes_copy,
    ) = local

    def up_copy(chunk):
        first = mine_g * share + chunk * chunk_cols
        return pltpu.make_async_copy(
            up_hbm.at[:, pl.ds(pl.multiple_of(first, chunk_cols), chunk_cols)],
            up.at[chunk],
            up_sem.at[chunk],
        )

    def down_copy(block, part):
        first = mine_g * share + part * piece
        return pltpu.make_async_copy(
            down_hbm.at[
                pl.ds(pl.multiple_of(first, piece), piece),
                pl.ds(block * block_cols, block_cols),
            ],
            down.at[block, pl.ds(part * piece, piece), :],
            down_sem.at[block * pieces + part],
        )

    chunk_copies = [up_copy(c) for c in range(up_chunks)] + [shared_down_copy] + [
        down_copy(b, p) for b in range(blocks) for p in range(pieces)
    ]
    issued = 0

    def start_chunks(last):
        nonlocal issued
        while issued < min(last, len(chunk_copies)):
            chunk_copies[issued].start(priority=PRIORITY)
            issued += 1

    for copy in (query_copy, key_new_copy, keys_copy, values_copy, value_new_copy, hidden_copy, lengths_copy, routes_copy, w_out_copy, gain_copy, router_copy, shared_up_copy):
        copy.start()
    start_chunks(EARLY)

    def loop(count, step):
        if count <= UNROLL:
            for i in range(count):
                step(i)
        else:

            def body(i, carry):
                step(i)
                return carry

            lax.fori_loop(0, count, body, 0)

    def other_group(off):
        return lax.rem(mine_g + off, replicas)

    def other_device(i):
        return i + jnp.where(i >= me, 1, 0)

    def greet(to):
        pl.semaphore_signal(barrier, inc=1, device_id=to, device_id_type=MESH)

    loop(n - 1, lambda i: greet({"expert": other_device(i)}))
    for off in range(1, replicas):
        greet({"group": other_group(off)})

    rows = lax.broadcasted_iota(jnp.int32, (HEADS, width), 0)
    lanes = lax.broadcasted_iota(jnp.int32, (HEADS, width), 1)
    own_lane = lanes // HEAD_DIM == rows

    def fold(x):
        row = lax.broadcasted_iota(jnp.int32, (HEADS, HEAD_DIM), 0)
        taken = jnp.zeros((HEADS, HEAD_DIM), F32)
        for h in range(HEADS):
            taken = taken + jnp.where(row == h, x[:, h * HEAD_DIM : (h + 1) * HEAD_DIM], 0.0)
        return taken

    scale = 1.0 / math.sqrt(HEAD_DIM)
    query_copy.wait()
    key_new_copy.wait()
    spread_query = jnp.where(
        own_lane, jnp.broadcast_to(query[...].astype(F32), (HEADS, width)), 0.0
    )
    own_score = (
        jnp.sum(spread_query * key_new[...].astype(F32), axis=1, keepdims=True) * scale
    )
    spread_query = spread_query.astype(BF16)
    mine = pl.ds(pl.multiple_of(me * HEADS, HEADS), HEADS)
    hidden_copy.wait()
    hidden_all[mine, :] = fold(
        jnp.broadcast_to(hidden[...].astype(F32), (HEADS, width))
    ).astype(BF16)
    keys_copy.wait()
    scores = (
        lax.dot_general(
            spread_query, keys[...], (((1,), (1,)), ((), ())), preferred_element_type=F32
        )
        * scale
    )
    lengths_copy.wait()
    values_copy.wait()
    value_new_copy.wait()
    start_chunks(len(chunk_copies))

    position = lax.broadcasted_iota(jnp.int32, scores.shape, 1)
    scores = jnp.where(position < lengths_ref[0], scores, -1e30)
    top = jnp.maximum(jnp.max(scores, axis=1, keepdims=True), own_score)
    weights = jnp.exp(scores - top)
    own_weight = jnp.exp(own_score - top)
    normalizer = jnp.sum(weights, axis=1, keepdims=True) + own_weight
    weights = (weights / normalizer).astype(BF16)
    own_weight = (own_weight / normalizer).astype(BF16).astype(F32)
    mixed = jnp.dot(weights, values[...], preferred_element_type=F32)
    mixed = mixed + own_weight * value_new[...].astype(F32)
    attended_all[mine, :] = fold(mixed).astype(BF16)
    routes_copy.wait()

    pl.semaphore_wait(barrier, n - 1 + replicas - 1)

    def send(src, dst, sem, to):
        pltpu.make_async_remote_copy(
            src_ref=src,
            dst_ref=dst,
            send_sem=send_sem.at[sem],
            recv_sem=recv_sem.at[sem],
            device_id=to,
            device_id_type=MESH,
        ).start()

    def send_group(ref, sem):
        loop(n - 1, lambda i: send(ref, ref, sem, {"expert": other_device(i)}))

    def await_bytes(ref, sem):
        pltpu.make_async_copy(ref, ref, sem).wait()

    attended_piece = attended_all.at[mine, :]
    send_group(attended_piece, 0)
    send_group(hidden_all.at[mine, :], 1)
    for off in range(1, replicas):
        send(routes_all.at[mine_g], routes_all.at[mine_g], 2, {"group": other_group(off)})

    for off in range(1, replicas):
        pl.semaphore_signal(
            ready_sem, inc=1, device_id={"group": other_group(off)}, device_id_type=MESH
        )

    square = (n, n)
    down_index = lax.broadcasted_iota(jnp.int32, square, 0)
    across_index = lax.broadcasted_iota(jnp.int32, square, 1)

    def placed(group):
        across = jnp.broadcast_to(routes_all[group].astype(F32), square)
        route = jnp.sum(
            jnp.where(down_index == across_index, across, 0.0), axis=1, keepdims=True
        )
        same = jnp.broadcast_to(route, square) == across
        slot_down = jnp.sum(
            jnp.where(same & (across_index < down_index), 1.0, 0.0), axis=1, keepdims=True
        )
        slot_across = jnp.sum(
            jnp.where(same & (down_index < across_index), 1.0, 0.0), axis=0, keepdims=True
        )
        return route, slot_down, across[0:1, :], slot_across

    route, slot_down, route_across, slot_across = placed(mine_g)

    def picks(expert, slot):
        wanted = jnp.broadcast_to(route_across, expert.shape) == expert.astype(F32)
        ranked = jnp.broadcast_to(slot_across, slot.shape) == slot.astype(F32)
        return jnp.where(wanted & ranked, 1.0, 0.0).astype(BF16)

    def picks_for_device(group):
        slot = lax.broadcasted_iota(jnp.int32, (served, n), 0)
        expert = jnp.full((served, n), expert_of(group, me), jnp.int32)
        return picks(expert, jnp.where(slot < slots, slot, n))

    def picks_for_group(group):
        row = lax.broadcasted_iota(jnp.int32, (n * slots, n), 0)
        return picks(expert_of(group, row // slots), row - row // slots * slots)

    own_picks = picks_for_device(mine_g)
    twin_picks = [picks_for_device(other_group(off)) for off in range(1, replicas)]
    group_picks = [picks_for_group(other_group(off)) for off in range(1, replicas)]
    guests_ref[...] = jnp.zeros(guests_ref.shape, F32)

    def unfolded(folded):
        unfold[...] = folded[...].astype(F32)
        return [unfold[pl.ds(h, n, stride=HEADS), :].astype(BF16) for h in range(HEADS)]

    others = pl.ds(0, (n - 1) * HEADS)
    twins = pl.ds(0, replicas - 1)
    w_out_copy.wait()
    await_bytes(attended_all.at[others, :], recv_sem.at[0])
    attended = jnp.concatenate(unfolded(attended_all), axis=1)
    projected = jnp.dot(attended, w_out[...], preferred_element_type=F32).astype(BF16)
    my_cols = pl.ds(pl.multiple_of(me * cols, cols), cols)
    if cols % 128 == 0:
        projected_all[:, my_cols] = projected
        piece_ref = projected_all.at[:, my_cols]
        near = projected_all.at[:, pl.ds(0, (n - 1) * cols)]
    else:
        projected_all[me] = projected
        piece_ref = projected_all.at[me]
        near = projected_all.at[pl.ds(0, n - 1)]
    for off in range(1, replicas):
        picked = jnp.dot(group_picks[off - 1], projected, preferred_element_type=F32)
        for j in range(n):
            picked_projected[off - 1, j] = picked[j * slots : (j + 1) * slots, :]
        group = other_group(off)
        if off == 1:
            pl.semaphore_wait(ready_sem, replicas - 1)
        loop(
            n,
            lambda j: send(
                picked_projected.at[off - 1, j],
                guest_projected.at[off - 1, me],
                4,
                {"group": group, "expert": j},
            ),
        )
    send_group(piece_ref, 3)
    await_bytes(hidden_all.at[others, :], recv_sem.at[1])
    every_hidden = jnp.concatenate(unfolded(hidden_all), axis=1)
    for off in range(1, replicas):
        picked_hidden[off - 1] = jnp.dot(
            twin_picks[off - 1], every_hidden, preferred_element_type=F32
        )[:slots, :]
        send(
            picked_hidden.at[off - 1],
            guest_hidden.at[off - 1],
            5,
            {"group": other_group(off)},
        )

    await_bytes(routes_all.at[twins], recv_sem.at[2])
    my_expert = expert_of(mine_g, me).astype(F32)

    def places(their_route, their_slot):
        here = their_route == my_expert
        return [jnp.where(here & (their_slot == float(k)), 1.0, 0.0) for k in range(slots)]

    token_places = [places(route, slot_down)]
    for off in range(1, replicas):
        their_route, their_slot, _, _ = placed(other_group(replicas - off))
        token_places.append(places(their_route, their_slot))
    gain_copy.wait()
    router_copy.wait()
    gain_row = gain[...].astype(F32).reshape(1, width)
    router_row = jnp.sum(
        jnp.where(
            lax.broadcasted_iota(jnp.int32, (EXPERTS, width), 0) == expert_of(mine_g, me),
            router[...].astype(F32),
            0.0,
        ),
        axis=0,
        keepdims=True,
    )

    def norm(residual):
        centered = residual - jnp.mean(residual, axis=1, keepdims=True)
        variance = jnp.mean(centered * centered, axis=1, keepdims=True)
        return centered / jnp.sqrt(jnp.maximum(variance, 0.25)) * gain_row

    token = lax.broadcasted_iota(jnp.int32, (n, 1), 0)
    shared_up_copy.wait()
    for chunk in range(up_chunks):
        up_copy(chunk).wait()
    await_bytes(near, recv_sem.at[3])
    if cols % 128 == 0:
        every_projected = projected_all[...].astype(F32)
    else:
        every_projected = jnp.concatenate([projected_all[d].astype(F32) for d in range(n)], axis=1)
    residual = every_hidden.astype(F32) + every_projected
    normed = norm(residual).astype(BF16)
    own_served = jnp.dot(own_picks, normed, preferred_element_type=F32)
    own_ref[...] = jnp.sum(jnp.where(token == me, residual, 0.0), axis=0, keepdims=True)
    shared_ref[...] = gelu(
        jnp.dot(normed, shared_up[...], preferred_element_type=F32)
    ).astype(BF16)

    await_bytes(guest_hidden, recv_sem.at[5])
    await_bytes(guest_projected, recv_sem.at[4])
    for off in range(1, replicas):
        theirs = jnp.concatenate([guest_projected[off - 1, d] for d in range(n)], axis=1)
        guests_ref[pl.ds(off * slots, slots), :] = norm(guest_hidden[off - 1] + theirs)
    everyone = (own_served + guests_ref[...]).astype(BF16)
    normed_ref[...] = everyone
    chosen = jnp.sum(everyone.astype(F32) * router_row, axis=1, keepdims=True)
    gate_ref[...] = 1.0 / (1.0 + jnp.exp(-chosen))
    for chunk in range(up_chunks):
        act = gelu(jnp.dot(normed_ref[...], up[chunk], preferred_element_type=F32))
        inner[:, pl.ds(chunk * chunk_cols, chunk_cols)] = act.astype(BF16)

    group_rows = GROUP_COLS // 128
    groups = width // GROUP_COLS
    blocks_per_group = blocks // groups
    shared_down_copy.wait()

    for group in range(groups):
        for index in range(blocks_per_group):
            block = group * blocks_per_group + index
            if block % 2 == 0:
                for later in range(block, min(block + 2, blocks)):
                    for part in range(pieces):
                        down_copy(later, part).wait()
            acc = gate_ref[...] * jnp.dot(inner[...], down[block], preferred_element_type=F32)
            terms = []
            for side in range(replicas):
                if side == 0:
                    total = jnp.dot(
                        shared_ref[...],
                        shared_down[:, pl.ds(block * block_cols, block_cols)],
                        preferred_element_type=F32,
                    )
                else:
                    total = jnp.zeros((n, block_cols), F32)
                for k in range(slots):
                    row = side * slots + k
                    total = total + token_places[side][k] * acc[row : row + 1, :]
                terms.append(total)
            for side in range(replicas):
                for k in range(block_cols // 128):
                    row = side * n * group_rows + index * (block_cols // 128) + k
                    terms_buf[pl.ds(row, n, stride=group_rows), :] = terms[side][
                        :, k * 128 : (k + 1) * 128
                    ]
        send_buf[group] = terms_buf[...].reshape(world, group_rows, 128).astype(BF16)

        def send_terms(i, group=group):
            def to(side, device):
                where = side * n
                send(
                    send_buf.at[group, where + device],
                    recv_buf.at[group, where + me],
                    6 + group,
                    {"group": other_group(replicas - side), "expert": device},
                )

            for side in range(1, replicas):
                to(side, i)
            if isinstance(i, int):
                if i < n - 1:
                    to(0, other_device(i))
            else:

                @pl.when(i < n - 1)
                def _():
                    to(0, other_device(i))

        loop(n, send_terms)
        recv_buf[group, me] = send_buf[group, me]

    for group in range(groups):
        landed = recv_buf.at[group, pl.ds(0, world - 1)]
        await_bytes(landed, recv_sem.at[6 + group])
        summed = jnp.zeros((group_rows, 128), F32)
        for d in range(world):
            summed = summed + recv_buf[group, d].astype(F32)
        for j in range(group_rows):
            where = pl.ds(group * GROUP_COLS + j * 128, 128)
            out_ref[:, where] = (own_ref[:, where] + summed[j : j + 1, :]).astype(out_ref.dtype)

    await_bytes(attended_all.at[others, :], send_sem.at[0])
    await_bytes(hidden_all.at[others, :], send_sem.at[1])
    await_bytes(routes_all.at[twins], send_sem.at[2])
    await_bytes(near, send_sem.at[3])
    await_bytes(guest_projected, send_sem.at[4])
    await_bytes(guest_hidden, send_sem.at[5])
    for group in range(groups):
        sent = send_buf.at[group, pl.ds(0, world - 1)]
        await_bytes(sent, send_sem.at[6 + group])


def solution(mesh):
    n = mesh.shape["expert"]
    replicas = mesh.shape["group"]
    world = n * replicas

    def body(
        query,
        key_new,
        value_new,
        key_cache,
        value_cache,
        lengths,
        hidden,
        routes,
        w_out,
        ln_gain,
        router,
        shared_up,
        shared_down,
        expert_up,
        expert_down,
    ):
        assert query.shape[0] == 1
        width = query.shape[1]
        share = expert_up.shape[1] // replicas
        cache = key_cache.shape[1]
        shared_units = shared_up.shape[1]
        cols = w_out.shape[1]
        slots = max(1, n // MOST_ROUTED)
        served = -(-slots * replicas // 16) * 16
        chunk_cols = min(CHUNK, share)
        up_chunks = share // chunk_cols
        blocks = width // BLOCK
        pieces = share // min(share, width)
        groups = width // GROUP_COLS
        rows_sent = GROUP_COLS // 128
        gathered = (n, width) if cols % 128 == 0 else (n, n, cols)
        vmem = pltpu.VMEM
        hbm = pl.BlockSpec(memory_space=pl.ANY)
        return pl.pallas_call(
            functools.partial(kernel, replicas, n),
            out_shape=pltpu.VMEM((1, width), BF16),
            in_specs=[hbm] * 15,
            out_specs=pl.BlockSpec(memory_space=pltpu.VMEM),
            scratch_shapes=[
                pltpu.SMEM(lengths.shape, jnp.int32),
                vmem((replicas, 1, n), jnp.int32),
                vmem((1, width), BF16),
                vmem((1, width), BF16),
                vmem((1, width), BF16),
                vmem((1, width), BF16),
                vmem((width,), BF16),
                vmem((cache, width), BF16),
                vmem((cache, width), BF16),
                vmem((width, cols), BF16),
                vmem((EXPERTS, width), BF16),
                vmem((width, shared_units), BF16),
                vmem((shared_units, width), BF16),
                vmem((up_chunks, width, chunk_cols), BF16),
                vmem((blocks, share, BLOCK), BF16),
                vmem((n * HEADS, HEAD_DIM), BF16),
                vmem((n * HEADS, HEAD_DIM), BF16),
                vmem((n * HEADS, HEAD_DIM), F32),
                vmem(gathered, BF16),
                vmem((replicas - 1, slots, width), F32),
                vmem((replicas - 1, slots, width), F32),
                vmem((replicas - 1, n, slots, cols), F32),
                vmem((replicas - 1, n, slots, cols), F32),
                vmem((served, width), F32),
                vmem((served, share), BF16),
                vmem((served, width), BF16),
                vmem((served, 1), F32),
                vmem((n, shared_units), BF16),
                vmem((1, width), F32),
                vmem((world * rows_sent, 128), F32),
                vmem((groups, world, rows_sent, 128), BF16),
                vmem((groups, world, rows_sent, 128), BF16),
                pltpu.SemaphoreType.DMA((13,)),
                pltpu.SemaphoreType.DMA((up_chunks,)),
                pltpu.SemaphoreType.DMA((blocks * pieces,)),
                pltpu.SemaphoreType.DMA((6 + groups,)),
                pltpu.SemaphoreType.DMA((6 + groups,)),
                pltpu.SemaphoreType.REGULAR,
            ],
            compiler_params=pltpu.CompilerParams(
                collective_id=0, has_side_effects=True, vmem_limit_bytes=66_900_000
            ),
        )(
            lengths,
            routes.reshape(1, n),
            query,
            key_new,
            value_new,
            hidden,
            ln_gain,
            key_cache.reshape(cache, width),
            value_cache.reshape(cache, width),
            w_out,
            router.T,
            shared_up,
            shared_down,
            expert_up,
            expert_down,
        )

    rows = P(("group", "expert"), None)
    placed = (
        rows,
        rows,
        rows,
        P(("group", "expert"), None, None),
        P(("group", "expert"), None, None),
        P(("group", "expert")),
        rows,
        P("group"),
        P(None, "expert"),
        P(),
        P(),
        P(None, "expert"),
        P("expert", None),
        P(None, "expert"),
        P("expert", None),
    )
    return jax.shard_map(body, mesh=mesh, in_specs=placed, out_specs=rows, check_vma=False)
```
